32 devices in a mesh: level: 4 (over z), dev: 8 (over y, x, core).
Axes of the slice: x: 2, y: 2, z: 4, core: 2. Of those that a mesh axis runs over, the one named last changes fastest.
Arguments:
- fields: float32 [4, 128, 12, 128], P('level', 'dev'), may hold values from -6 to 6
- own_src: int32 [4, 128], P('level', 'dev'), may hold values from 0 to 15
- own_weight: bfloat16 [4, 128, 128, 128], P('level', 'dev'), may hold values from 0 to 1, as said below
- send_block: int32 [4, 8, 8, 2], P('level', 'dev'), may hold values from 0 to 15
- send_target: int32 [4, 8, 8, 2], P('level', 'dev'), may hold values from 0 to 15
- send_count: int32 [4, 8, 8], P('level', 'dev'), may hold values from 0 to 2, as said below
- send_weight: bfloat16 [4, 8, 8, 2, 128, 128], P('level', 'dev'), may hold values from 0 to 1, as said below
- left_block: int32 [4, 8, 4, 2], P('level', 'dev'), may hold values from 0 to 15
- left_target: int32 [4, 8, 4, 2], P('level', 'dev'), may hold values from 0 to 15
- left_count: int32 [4, 8, 4], P('level', 'dev'), may hold values from 0 to 2, as said below
- left_weight: bfloat16 [4, 8, 4, 2, 128, 128], P('level', 'dev'), may hold values from 0 to 1, as said below
Outputs:
- remapped: float32 [4, 128, 12, 128], P('level', 'dev')
- totals: float32 [12], replicated
The draws below stay inside these ranges and needn't reach their ends.
Inputs may be any that keep to these rules, and one draw needn't show every extreme that they name: send_count[l, s, s] = 0; for every level some receiver device gets 2 live slots from every other device of the level. left_count[m, q, m] = 0; for every device index some receiver level gets 2 live slots from every other level. `own_weight`: nonnegative; entry [k, i] is zero where old cell k and new cell i differ by more than 3; each column sums to a positive intersect fraction of at most 1. `send_weight`: nonnegative; entry [k, i] is zero where old cell k and new cell i differ by more than 3; each column sums to a positive intersect fraction of at most 1. `left_weight`: nonnegative; entry [k, i] is zero where old cell k and new cell i differ by more than 3; each column sums to a positive intersect fraction of at most 1.
All inputs are finite; a program needn't handle non-finite values.
Results may differ from the reference program's by a relative error of at most 0.0045.
Values may be sent and summed in bfloat16 or wider, within the bound.
No kernel may reach another device: no remote copies, remote signals or barrier semaphores. Data moves between devices by JAX's collectives and lax.ppermute only.
A program may use at most 64 MiB of HBM per device.

```python
import jax
import jax.numpy as jnp
from jax import lax

COMP = 12
CELLS = 128
HALF = 3
BLK_DEV = 16
CAP = 2
LCAP = 2
PEERS = 8
LEVELS = 4
BLOCKS = 128


def band_fractions(key, lead):
    first, second, third = jax.random.split(key, 3)
    shape = lead + (CELLS, CELLS)
    rowpos = lax.broadcasted_iota(jnp.int32, shape, len(lead))
    colpos = lax.broadcasted_iota(jnp.int32, shape, len(lead) + 1)
    spread = jnp.abs(rowpos - colpos)
    middle = jax.random.uniform(first, shape, jnp.float32, 2.0, 3.0)
    beside = jax.random.uniform(second, shape, jnp.float32, 0.3, 1.0)
    raw = jnp.where(spread == 0, middle, jnp.where(spread <= HALF, beside, jnp.zeros_like(beside)))
    fraction = jax.random.uniform(third, lead + (1, CELLS), jnp.float32, 0.2, 0.8)
    return raw / jnp.sum(raw, axis=-2, keepdims=True) * fraction


def draw_own_weight(key, part):
    whole = band_fractions(jax.random.fold_in(key, 11), (LEVELS, BLOCKS))
    return whole.astype(jnp.bfloat16)


def draw_send_weight(key, part):
    whole = band_fractions(jax.random.fold_in(key, 23), (LEVELS, PEERS, PEERS, CAP))
    return whole.astype(jnp.bfloat16)


def draw_left_weight(key, part):
    whole = band_fractions(jax.random.fold_in(key, 37), (LEVELS, PEERS, LEVELS, LCAP))
    return whole.astype(jnp.bfloat16)


def draw_send_count(key, part):
    shape = (LEVELS, PEERS, PEERS)
    base = jax.random.randint(key, shape, 0, CAP + 1)
    lvl = lax.broadcasted_iota(jnp.int32, shape, 0)
    src = lax.broadcasted_iota(jnp.int32, shape, 1)
    dst = lax.broadcasted_iota(jnp.int32, shape, 2)
    heavy = (7 * lvl + 3) % PEERS
    near = ((dst - src) % PEERS == 1) | ((src - dst) % PEERS == 1)
    full = (dst == heavy) | near
    out = jnp.where(full, CAP, base)
    return jnp.where(src == dst, 0, out).astype(jnp.int32)


def draw_left_count(key, part):
    shape = (LEVELS, PEERS, LEVELS)
    base = jax.random.randint(key, shape, 0, LCAP + 1)
    src = lax.broadcasted_iota(jnp.int32, shape, 0)
    dev = lax.broadcasted_iota(jnp.int32, shape, 1)
    dst = lax.broadcasted_iota(jnp.int32, shape, 2)
    heavy = (5 * dev + 1) % LEVELS
    near = ((dst - src) % LEVELS == 1) | ((src - dst) % LEVELS == 1)
    full = (dst == heavy) | near
    out = jnp.where(full, LCAP, base)
    return jnp.where(src == dst, 0, out).astype(jnp.int32)


def with_ends(drawn, own_key, smallest, top_value):
    spot = [jax.random.randint(jax.random.fold_in(own_key, axis), (), 0, length) for axis, length in enumerate(drawn.shape)]
    widest = drawn.shape.index(max(drawn.shape))
    next_to = spot[:widest] + [(spot[widest] + 1) % drawn.shape[widest]] + spot[widest + 1:]
    return drawn.at[tuple(spot)].set(smallest).at[tuple(next_to)].set(top_value)


def block_levels(key, shape, cuts, smallest, top_value):
    def one(position, parts):
        steps = jax.random.uniform(jax.random.fold_in(jax.random.fold_in(key, 6), position), (parts,), jnp.float32, smallest / len(cuts), top_value / len(cuts))
        return jnp.repeat(jnp.exp(steps), shape[position] // parts).reshape((-1,) + (1,) * (len(shape) - position - 1))

    loudness = one(*cuts[0])
    for cut in cuts[1:]:
        loudness = loudness * one(*cut)
    return loudness


def centred(rng, dims, deviation, reach, cuts=(), dtype=jnp.bfloat16):
    result = deviation * jax.random.normal(rng, dims, jnp.float32)
    if cuts:
        result = result * block_levels(rng, dims, cuts, -0.22, 0.18)
    return jnp.clip(result, -reach, reach).astype(dtype)


def setup_inputs(seed: int = 0) -> dict:
    splits = jax.random.split(jax.random.key(seed), 12)
    fields = centred(splits[0], (LEVELS, BLOCKS, COMP, CELLS), 1.0, 6.0, ((0, 4), (1, 8)), jnp.float32)
    own_src = with_ends(jax.random.randint(splits[1], (LEVELS, BLOCKS), 0, BLK_DEV), jax.random.fold_in(splits[1], 1), 0, BLK_DEV - 1).astype(jnp.int32)
    own_weight = draw_own_weight(jax.random.fold_in(splits[11], 71), 0)
    send_block = with_ends(jax.random.randint(splits[3], (LEVELS, PEERS, PEERS, CAP), 0, BLK_DEV), jax.random.fold_in(splits[3], 1), 0, BLK_DEV - 1).astype(jnp.int32)
    send_target = with_ends(jax.random.randint(splits[4], (LEVELS, PEERS, PEERS, CAP), 0, BLK_DEV), jax.random.fold_in(splits[4], 1), 0, BLK_DEV - 1).astype(jnp.int32)
    send_count = draw_send_count(jax.random.fold_in(splits[11], 71), 0)
    send_weight = draw_send_weight(jax.random.fold_in(splits[11], 71), 0)
    left_block = with_ends(jax.random.randint(splits[7], (LEVELS, PEERS, LEVELS, LCAP), 0, BLK_DEV), jax.random.fold_in(splits[7], 1), 0, BLK_DEV - 1).astype(jnp.int32)
    left_target = with_ends(jax.random.randint(splits[8], (LEVELS, PEERS, LEVELS, LCAP), 0, BLK_DEV), jax.random.fold_in(splits[8], 1), 0, BLK_DEV - 1).astype(jnp.int32)
    left_count = draw_left_count(jax.random.fold_in(splits[11], 71), 0)
    left_weight = draw_left_weight(jax.random.fold_in(splits[11], 71), 0)
    return dict(fields=fields, own_src=own_src, own_weight=own_weight, send_block=send_block, send_target=send_target, send_count=send_count, send_weight=send_weight, left_block=left_block, left_target=left_target, left_count=left_count, left_weight=left_weight)


def reference(fields, own_src, own_weight, send_block, send_target, send_count, send_weight, left_block, left_target, left_count, left_weight):
    levels = fields.shape[0]
    peers = send_count.shape[1]
    blocks = fields.shape[1] // peers
    comp = fields.shape[2]
    cells = fields.shape[3]
    rounded = fields.astype(jnp.bfloat16).reshape(levels, peers, blocks, comp, cells)
    highest = lax.Precision.HIGHEST

    own_index = own_src.reshape(levels, peers, blocks, 1, 1).astype(jnp.int32)
    own_donor = jnp.take_along_axis(rounded, own_index, axis=2).astype(jnp.float32)
    own_frac = own_weight.reshape(levels, peers, blocks, cells, cells).astype(jnp.float32)
    own = jnp.einsum("lqbmk,lqbki->lqbmi", own_donor, own_frac, precision=highest)

    source_dev = lax.broadcasted_iota(jnp.int32, (peers, 1, 1), 0)
    recv_dev = lax.broadcasted_iota(jnp.int32, (1, peers, 1), 1)
    slot_cap = send_block.shape[3]

    def level_intra(packed):
        flds, blk, tgt, cnt, wts = packed
        donors = flds[source_dev, blk]
        valid = lax.broadcasted_iota(jnp.int32, (1, 1, slot_cap), 2) < cnt[:, :, None]
        donors = jnp.where(valid[..., None, None], donors, jnp.zeros_like(donors))
        contrib = jnp.einsum("spcmk,spcki->spcmi", donors.astype(jnp.float32), wts.astype(jnp.float32), precision=highest)
        receive = (recv_dev * blocks + tgt).reshape(-1).astype(jnp.int32)
        total = jnp.zeros((peers * blocks, comp, cells), jnp.float32)
        return total.at[receive].add(contrib.reshape(-1, comp, cells)).reshape(peers, blocks, comp, cells)

    intra = lax.map(level_intra, (rounded, send_block, send_target, send_count, send_weight))

    left_cap = left_block.shape[3]
    dev_index = lax.broadcasted_iota(jnp.int32, (peers, 1, 1), 0)

    def level_left(packed):
        flds, blk, cnt, wts = packed
        donors = flds[dev_index, blk]
        valid = lax.broadcasted_iota(jnp.int32, (1, 1, left_cap), 2) < cnt[:, :, None]
        donors = jnp.where(valid[..., None, None], donors, jnp.zeros_like(donors))
        return jnp.einsum("qlcmk,qlcki->qlcmi", donors.astype(jnp.float32), wts.astype(jnp.float32), precision=highest)

    left_terms = lax.map(level_left, (rounded, left_block, left_count, left_weight))
    dst_level = lax.broadcasted_iota(jnp.int32, (1, 1, levels, 1), 2)
    dev_here = lax.broadcasted_iota(jnp.int32, (1, peers, 1, 1), 1)
    recv_left = ((dst_level * peers + dev_here) * blocks + left_target).reshape(-1).astype(jnp.int32)
    leftover = jnp.zeros((levels * peers * blocks, comp, cells), jnp.float32)
    leftover = leftover.at[recv_left].add(left_terms.reshape(-1, comp, cells))
    leftover = leftover.reshape(levels, peers, blocks, comp, cells)

    remapped = (own + intra + leftover).reshape(levels, peers * blocks, comp, cells)
    totals = jnp.sum(remapped, axis=(0, 1, 3)) / (CELLS * BLK_DEV)
    return remapped, totals
```

```python
import functools

import jax
import jax.numpy as jnp
from jax import lax
from jax.experimental import pallas as pl
from jax.experimental.pallas import tpu as pltpu
from jax.sharding import PartitionSpec as P

LANES = 128
TILE = 16


def up(value, step):
    return -(-value // step) * step


class Plan:
    def __init__(self, levels, peers, blocks, comp, cells, cap, lcap):
        self.levels, self.peers, self.blocks = levels, peers, blocks
        self.comp, self.cells, self.cap, self.lcap = comp, cells, cap, lcap
        self.slots = max(cap, lcap)
        self.width = self.slots * TILE
        self.per_group = LANES // self.width
        self.dev_groups = -(-peers // self.per_group)
        self.lev_groups = -(-levels // self.per_group)
        self.groups = self.dev_groups + self.lev_groups
        spare = TILE - comp
        self.sum_row = comp
        if self.groups <= spare:
            self.target_row = (self.slots - 1) * TILE + comp
            self.rows = self.width
        else:
            self.target_row = self.width
            self.rows = self.width + up(self.groups, TILE)
        assert comp + 3 <= TILE and self.slots >= 2 and cells == LANES


def first_kernel(
    plan,
    fields_hbm,
    own_src_hbm,
    own_weight_hbm,
    send_block_hbm,
    send_target_hbm,
    send_count_hbm,
    send_weight_hbm,
    left_block_hbm,
    left_target_hbm,
    left_count_hbm,
    left_weight_hbm,
    own_ref,
    msg_ref,
    fields_v,
    donors,
    own_weight,
    send_weight,
    left_weight,
    own_src,
    send_block,
    send_target,
    send_count,
    left_block,
    left_target,
    left_count,
    sems,
):
    blocks, comp = plan.blocks, plan.comp
    pairs = (
        (fields_hbm, fields_v),
        (own_src_hbm, own_src),
        (send_block_hbm, send_block),
        (send_target_hbm, send_target),
        (send_count_hbm, send_count),
        (left_block_hbm, left_block),
        (left_target_hbm, left_target),
        (left_count_hbm, left_count),
        (send_weight_hbm, send_weight),
        (left_weight_hbm, left_weight),
        (own_weight_hbm, own_weight),
    )
    copies = [pltpu.make_async_copy(src, dst, sems.at[i]) for i, (src, dst) in enumerate(pairs)]
    for copy in copies:
        copy.start()

    level = lax.axis_index("level")
    dev = lax.axis_index("dev")
    row = lax.broadcasted_iota(jnp.int32, (TILE, LANES), 0)
    lane = lax.broadcasted_iota(jnp.int32, (TILE, LANES), 1)
    part = lane % plan.width // TILE
    group_lane = lane // plan.width

    copies[0].wait()
    donors[...] = jnp.zeros_like(donors)
    for b in range(blocks):
        donors[b, 0:comp, :] = fields_v[pl.ds(b, comp, stride=blocks), :].astype(jnp.bfloat16)
    for copy in copies[1:8]:
        copy.wait()

    def term(block, weight):
        return jnp.dot(donors[block], weight, preferred_element_type=jnp.float32)

    sums = jnp.zeros((TILE, LANES), jnp.float32)
    dev_terms = []
    copies[8].wait()
    for p in range(plan.peers):
        terms = []
        for c in range(plan.cap):
            block = jnp.where(c < send_count[0, p], send_block[c, p], blocks)
            terms.append(term(block, send_weight[p * plan.cap + c]))
            sums += terms[-1]
        dev_terms.append(terms)
    lev_terms = []
    copies[9].wait()
    for p in range(plan.levels):
        terms = []
        for c in range(plan.lcap):
            block = jnp.where(c < left_count[0, p], left_block[c, p], blocks)
            terms.append(term(block, left_weight[p * plan.lcap + c]))
            sums += terms[-1]
        lev_terms.append(terms)
    copies[10].wait()
    for b in range(blocks):
        mine = term(own_src[0, b], own_weight[b])
        sums += mine
        own_ref[pl.ds(b, comp, stride=blocks), :] = mine[0:comp]

    total = jnp.sum(sums, axis=1, keepdims=True)
    total = jnp.sum(jnp.where(row == lane, total, 0.0), axis=0, keepdims=True)
    high = total.astype(jnp.bfloat16).astype(jnp.float32)
    rest = total - high
    middle = rest.astype(jnp.bfloat16).astype(jnp.float32)
    low = rest - middle
    sum_rows = jnp.where(
        row == plan.sum_row,
        high,
        jnp.where(row == plan.sum_row + 1, middle, jnp.where(row == plan.sum_row + 2, low, 0.0)),
    )

    def target_tile(group, offset, targets, base):
        value = jnp.zeros((TILE, LANES), jnp.int32)
        for c, target in enumerate(targets):
            value = jnp.where(part == c, target, value)
        here = (row + base == plan.target_row + group) & (group_lane == offset)
        return jnp.where(here, value, 0).astype(jnp.float32)

    def write(index, terms, targets, group, offset):
        for c in range(plan.slots):
            data = terms[c] if c < len(terms) else jnp.zeros((TILE, LANES), jnp.float32)
            if c == 0:
                data = data + sum_rows
            if plan.target_row // TILE == c:
                data = data + target_tile(group, offset, targets, c * TILE)
            msg_ref[index, c * TILE : (c + 1) * TILE, :] = data.astype(jnp.bfloat16)
        for r in range(plan.width, plan.rows, TILE):
            msg_ref[index, r : r + TILE, :] = target_tile(group, offset, targets, r).astype(
                jnp.bfloat16
            )

    meta = sum_rows.astype(jnp.bfloat16)
    for index in range(plan.levels * plan.peers):
        msg_ref[index, 0:TILE, :] = meta
    for p in range(plan.peers):
        write(
            level * plan.peers + p,
            dev_terms[p],
            [send_target[c, p] for c in range(plan.cap)],
            dev // plan.per_group,
            dev % plan.per_group,
        )
    for p in range(plan.levels):
        write(
            p * plan.peers + dev,
            lev_terms[p],
            [left_target[c, p] for c in range(plan.lcap)],
            plan.dev_groups + level // plan.per_group,
            level % plan.per_group,
        )


def second_kernel(plan, own_ref, msg_ref, out_ref, totals_ref, picked):
    blocks, comp = plan.blocks, plan.comp
    level = lax.axis_index("level")
    dev = lax.axis_index("dev")

    def gather(first, count, index_of):
        targets = jnp.zeros((plan.rows - plan.target_row // TILE * TILE, LANES), jnp.float32)
        span = up(count, plan.per_group)
        for s in range(span):
            at = (first * plan.per_group + s) * plan.width
            if s < count:
                picked[at : at + plan.width, :] = msg_ref[index_of(s), 0 : plan.width, :]
                targets += msg_ref[
                    index_of(s), plan.target_row // TILE * TILE : plan.rows, :
                ].astype(jnp.float32)
            else:
                picked[at : at + plan.width, :] = jnp.zeros((plan.width, LANES), jnp.bfloat16)
        return targets

    dev_targets = gather(0, plan.peers, lambda s: level * plan.peers + s)
    lev_targets = gather(plan.dev_groups, plan.levels, lambda s: s * plan.peers + dev)

    block_row = lax.broadcasted_iota(jnp.int32, (blocks, LANES), 0).astype(jnp.float32)
    lane = lax.broadcasted_iota(jnp.int32, (blocks, LANES), 1)
    one = jnp.ones((blocks, LANES), jnp.float32)
    zero = jnp.zeros((blocks, LANES), jnp.float32)
    placed = jnp.zeros((comp * blocks, LANES), jnp.float32)
    for g in range(plan.groups):
        targets = dev_targets if g < plan.dev_groups else lev_targets
        r = plan.target_row % TILE + g
        match = jnp.where(block_row == targets[r : r + 1, :], one, zero)
        select = jnp.concatenate(
            [jnp.where(lane % TILE == m, match, zero) for m in range(comp)], axis=0
        ).astype(jnp.bfloat16)
        placed += jnp.dot(
            select, picked[g * LANES : (g + 1) * LANES, :], preferred_element_type=jnp.float32
        )
    out_ref[...] = own_ref[...] + placed

    sums = jnp.zeros((TILE, LANES), jnp.float32)
    for index in range(plan.levels * plan.peers):
        sums += msg_ref[index, 0:TILE, :].astype(jnp.float32)
    r = plan.sum_row
    total = sums[r : r + 1, :] + sums[r + 1 : r + 2, :] + sums[r + 2 : r + 3, :]
    totals_ref[...] = (total * (1.0 / (plan.cells * blocks)))[0, :comp]


def body(
    fields,
    own_src,
    own_weight,
    send_block,
    send_target,
    send_count,
    send_weight,
    left_block,
    left_target,
    left_count,
    left_weight,
):
    blocks, comp, cells = fields.shape[1:]
    peers, cap = send_block.shape[2:]
    levels, lcap = left_block.shape[2:]
    plan = Plan(levels, peers, blocks, comp, cells, cap, lcap)
    rows = comp * blocks
    in_hbm = pl.BlockSpec(memory_space=pltpu.HBM)
    vmem = pl.BlockSpec(memory_space=pltpu.VMEM)
    own, message = pl.pallas_call(
        functools.partial(first_kernel, plan),
        out_shape=(
            jax.ShapeDtypeStruct((rows, cells), jnp.float32),
            jax.ShapeDtypeStruct((levels * peers, plan.rows, cells), jnp.bfloat16),
        ),
        in_specs=[in_hbm] * 11,
        out_specs=(vmem, vmem),
        scratch_shapes=[
            pltpu.VMEM((rows, cells), jnp.float32),
            pltpu.VMEM((blocks + 1, TILE, cells), jnp.bfloat16),
            pltpu.VMEM((blocks, cells, cells), jnp.bfloat16),
            pltpu.VMEM((peers * cap, cells, cells), jnp.bfloat16),
            pltpu.VMEM((levels * lcap, cells, cells), jnp.bfloat16),
            pltpu.SMEM((1, blocks), jnp.int32),
            pltpu.SMEM((cap, peers), jnp.int32),
            pltpu.SMEM((cap, peers), jnp.int32),
            pltpu.SMEM((1, peers), jnp.int32),
            pltpu.SMEM((lcap, levels), jnp.int32),
            pltpu.SMEM((lcap, levels), jnp.int32),
            pltpu.SMEM((1, levels), jnp.int32),
            pltpu.SemaphoreType.DMA((11,)),
        ],
        compiler_params=pltpu.CompilerParams(vmem_limit_bytes=24 * 2**20),
        name="terms",
    )(*(pltpu.with_memory_space_constraint(x, pltpu.HBM) for x in (
        fields[0].transpose(1, 0, 2).reshape(rows, cells),
        own_src,
        own_weight[0],
        send_block[0, 0].T,
        send_target[0, 0].T,
        send_count[0],
        send_weight[0, 0].reshape(peers * cap, cells, cells),
        left_block[0, 0].T,
        left_target[0, 0].T,
        left_count[0],
        left_weight[0, 0].reshape(levels * lcap, cells, cells),
    )))
    message = lax.all_to_all(message, ("level", "dev"), split_axis=0, concat_axis=0, tiled=True)
    remapped, totals = pl.pallas_call(
        functools.partial(second_kernel, plan),
        out_shape=(
            jax.ShapeDtypeStruct((rows, cells), jnp.float32),
            jax.ShapeDtypeStruct((comp,), jnp.float32),
        ),
        in_specs=[vmem, vmem],
        out_specs=(vmem, vmem),
        scratch_shapes=[pltpu.VMEM((plan.groups * LANES, cells), jnp.bfloat16)],
        compiler_params=pltpu.CompilerParams(vmem_limit_bytes=24 * 2**20),
        name="place",
    )(own, message)
    remapped = remapped.reshape(comp, blocks, cells).transpose(1, 0, 2)
    return (remapped[None], totals)


def solution(mesh):
    in_specs = (
        P("level", "dev", None, None),
        P("level", "dev"),
        P("level", "dev", None, None),
        P("level", "dev", None, None),
        P("level", "dev", None, None),
        P("level", "dev", None),
        P("level", "dev", None, None, None, None),
        P("level", "dev", None, None),
        P("level", "dev", None, None),
        P("level", "dev", None),
        P("level", "dev", None, None, None, None),
    )
    out_specs = (P("level", "dev", None, None), P())
    return jax.shard_map(body, mesh=mesh, in_specs=in_specs, out_specs=out_specs, check_vma=False)
```

```python
import functools

import jax
import jax.numpy as jnp
from jax import lax
from jax.experimental import pallas as pl
from jax.experimental.pallas import tpu as pltpu
from jax.sharding import PartitionSpec as P

LANES = 128
TILE = 16


def divide(x, n, bound):
    if n & (n - 1) == 0:
        return x >> (n.bit_length() - 1)
    factor = -(-(1 << 20) // n)
    assert bound * (factor * n - (1 << 20)) < 1 << 20 and bound * factor < 1 << 31
    return (x * factor) >> 20


class Plan:
    def __init__(self, levels, peers, blocks, comp, cells, cap, lcap):
        self.levels, self.peers, self.blocks = levels, peers, blocks
        self.comp, self.cells, self.cap = comp, cells, cap
        self.data = cap * comp
        self.rows = self.data + 2
        self.ahead = peers * self.rows
        self.total = levels * self.ahead
        self.ids = (peers + levels) * cap
        self.groups = -(-self.total // LANES)
        assert cap == lcap and comp <= TILE and cells == LANES
        assert self.ahead % TILE == 0 and self.ids <= LANES
        assert self.rows % 2 == 0 and 2 * TILE + comp <= LANES

    def lane_of(self, level, dev, donor_level, peer, slot):
        other = jnp.where(peer == dev, (self.peers + donor_level) * self.cap + slot, -1)
        return jnp.where(donor_level == level, peer * self.cap + slot, other)

    def slot_of(self, row):
        slot = jnp.zeros_like(row)
        for c in range(1, self.cap):
            slot += jnp.where(row >= c * self.comp, 1, 0)
        return slot


def first_kernel(
    plan,
    fields_hbm,
    own_src_hbm,
    own_weight_hbm,
    send_block_hbm,
    send_target_hbm,
    send_count_hbm,
    send_weight_hbm,
    left_block_hbm,
    left_target_hbm,
    left_count_hbm,
    left_weight_hbm,
    own_ref,
    msg_ref,
    place_ref,
    fields_v,
    donors,
    own_weight,
    send_weight,
    left_weight,
    wide,
    own_src,
    send_block,
    send_target,
    send_count,
    left_block,
    left_target,
    left_count,
    sems,
):
    blocks, comp, cap = plan.blocks, plan.comp, plan.cap
    pairs = (
        (fields_hbm, fields_v),
        (own_src_hbm, own_src),
        (send_block_hbm, send_block),
        (send_target_hbm, send_target),
        (send_count_hbm, send_count),
        (left_block_hbm, left_block),
        (left_target_hbm, left_target),
        (left_count_hbm, left_count),
        (send_weight_hbm, send_weight),
        (left_weight_hbm, left_weight),
        (own_weight_hbm, own_weight),
    )
    copies = [pltpu.make_async_copy(src, dst, sems.at[i]) for i, (src, dst) in enumerate(pairs)]
    for copy in copies:
        copy.start()

    level = lax.axis_index("level")
    dev = lax.axis_index("dev")

    lane = lax.broadcasted_iota(jnp.int32, (1, LANES), 1)
    for g in range(plan.groups):
        at = lane + g * LANES
        index = divide(at, plan.rows, plan.total + LANES)
        row = at - index * plan.rows
        donor_level = divide(index, plan.peers, plan.levels * plan.peers + LANES)
        peer = index - donor_level * plan.peers
        slot = plan.slot_of(row)
        at_lane = plan.lane_of(level, dev, donor_level, peer, slot)
        part = jnp.where((at_lane >= 0) & (row < plan.data), row - slot * comp, -1)
        part = jnp.where(at < plan.total, part, -1)
        place_ref[g : g + 1, :] = jnp.maximum(at_lane, 0)
        place_ref[plan.groups + g : plan.groups + g + 1, :] = part

    wide[...] = jnp.zeros_like(wide)

    copies[0].wait()
    donors[...] = jnp.zeros_like(donors)
    for b in range(blocks):
        donors[b, 0:comp, :] = fields_v[pl.ds(b, comp, stride=blocks), :].astype(jnp.bfloat16)
    for copy in copies[1:8]:
        copy.wait()

    row = lax.broadcasted_iota(jnp.int32, (TILE, LANES), 0)
    column = lax.broadcasted_iota(jnp.int32, (TILE, LANES), 1)

    def term(block, weight):
        return jnp.dot(donors[block], weight, preferred_element_type=jnp.float32)

    sums = jnp.zeros((TILE, LANES), jnp.float32)
    for count, block, target, weight, peers, here, message_of, copy in (
        (
            send_count,
            send_block,
            send_target,
            send_weight,
            plan.peers,
            dev,
            lambda p: level * plan.peers + p,
            copies[8],
        ),
        (
            left_count,
            left_block,
            left_target,
            left_weight,
            plan.levels,
            plan.peers + level,
            lambda p: p * plan.peers + dev,
            copies[9],
        ),
    ):
        copy.wait()
        for p in range(peers):
            first = message_of(p) * plan.rows
            targets = jnp.zeros((1, LANES), jnp.float32)
            for c in range(cap):
                donor = jnp.where(c < count[0, p], block[c, p], blocks)
                value = term(donor, weight[p * cap + c])
                sums += value
                wide[pl.ds(first + c * comp, comp), :] = value[0:comp]
                targets = jnp.where(
                    lane == here * cap + c, target[c, p].astype(jnp.float32), targets
                )
            wide[pl.ds(first + plan.data, 1), :] = targets
    copies[10].wait()
    for b in range(blocks):
        mine = term(own_src[0, b], own_weight[b])
        sums += mine
        own_ref[pl.ds(b, comp, stride=blocks), :] = mine[0:comp]

    total = jnp.sum(sums, axis=1, keepdims=True)
    high = total.astype(jnp.bfloat16).astype(jnp.float32)
    rest = total - high
    middle = rest.astype(jnp.bfloat16).astype(jnp.float32)
    low = rest - middle
    spread = jnp.where(column == row, high, 0.0)
    spread = jnp.where(column == row + TILE, middle, spread)
    spread = jnp.where(column == row + 2 * TILE, low, spread)
    sum_row = jnp.sum(spread, axis=0, keepdims=True)
    for index in range(plan.levels * plan.peers):
        at = index * plan.rows + plan.data + 1
        wide[at : at + 1, :] = sum_row
    msg_ref[...] = wide[...].astype(jnp.bfloat16)


def second_kernel(plan, own_ref, msg_ref, place_ref, out_ref, totals_ref):
    blocks, comp = plan.blocks, plan.comp
    spans = [
        (g, g * LANES, min(LANES, plan.total - g * LANES)) for g in range(plan.groups)
    ]

    found = {}
    for peer in range(plan.peers):
        at = peer * plan.rows + plan.data
        low = at // 8 * 8
        for donor_level in range(plan.levels):
            first = donor_level * plan.ahead + low
            part = msg_ref[first : first + 8, :].astype(jnp.float32)
            found[at - low] = found[at - low] + part if at - low in found else part
    meta = sum(part[at : at + 2, :] for at, part in found.items())

    targets = jnp.broadcast_to(meta[0:1, :], (blocks, LANES))
    block_row = lax.broadcasted_iota(jnp.int32, (blocks, LANES), 0).astype(jnp.float32)
    placed = own_ref[...]
    for g, at, size in spans:
        index = jnp.broadcast_to(place_ref[g : g + 1, :], (blocks, LANES))
        match = jnp.take_along_axis(targets, index, axis=1) == block_row
        at_part = plan.groups + g
        part = jnp.broadcast_to(place_ref[at_part : at_part + 1, :], (blocks, LANES))
        key = jnp.where(match, part, -1)
        select = jnp.concatenate(
            [jnp.where(key == m, 1.0, 0.0).astype(jnp.bfloat16) for m in range(comp)], axis=0
        )
        placed += jnp.dot(
            select[:, :size], msg_ref[at : at + size, :], preferred_element_type=jnp.float32
        )
    out_ref[...] = placed

    sums = meta[1:2, :]
    total = sums[:, 0:comp]
    total += sums[:, TILE : TILE + comp]
    total += sums[:, 2 * TILE : 2 * TILE + comp]
    totals_ref[...] = (total * (1.0 / (plan.cells * blocks)))[0]


def hbm(x):
    return pltpu.with_memory_space_constraint(x, pltpu.HBM)


def body(
    fields,
    own_src,
    own_weight,
    send_block,
    send_target,
    send_count,
    send_weight,
    left_block,
    left_target,
    left_count,
    left_weight,
):
    blocks, comp, cells = fields.shape[1:]
    peers, cap = send_block.shape[2:]
    levels, lcap = left_block.shape[2:]
    plan = Plan(levels, peers, blocks, comp, cells, cap, lcap)
    rows = comp * blocks
    devices = levels * peers
    in_hbm = pl.BlockSpec(memory_space=pltpu.HBM)
    vmem = pl.BlockSpec(memory_space=pltpu.VMEM)
    own, message, place = pl.pallas_call(
        functools.partial(first_kernel, plan),
        out_shape=(
            jax.ShapeDtypeStruct((rows, cells), jnp.float32),
            jax.ShapeDtypeStruct((plan.total, cells), jnp.bfloat16),
            jax.ShapeDtypeStruct((2 * plan.groups, LANES), jnp.int32),
        ),
        in_specs=[in_hbm] * 11,
        out_specs=(vmem, vmem, vmem),
        scratch_shapes=[
            pltpu.VMEM((rows, cells), jnp.float32),
            pltpu.VMEM((blocks + 1, TILE, cells), jnp.bfloat16),
            pltpu.VMEM((blocks, cells, cells), jnp.bfloat16),
            pltpu.VMEM((peers * cap, cells, cells), jnp.bfloat16),
            pltpu.VMEM((levels * lcap, cells, cells), jnp.bfloat16),
            pltpu.VMEM((plan.total, cells), jnp.float32),
            pltpu.SMEM((1, blocks), jnp.int32),
            pltpu.SMEM((cap, peers), jnp.int32),
            pltpu.SMEM((cap, peers), jnp.int32),
            pltpu.SMEM((1, peers), jnp.int32),
            pltpu.SMEM((lcap, levels), jnp.int32),
            pltpu.SMEM((lcap, levels), jnp.int32),
            pltpu.SMEM((1, levels), jnp.int32),
            pltpu.SemaphoreType.DMA((11,)),
        ],
        compiler_params=pltpu.CompilerParams(vmem_limit_bytes=24 * 2**20),
        name="terms",
    )(
        hbm(fields[0].transpose(1, 0, 2).reshape(rows, cells)),
        hbm(own_src),
        hbm(own_weight[0]),
        hbm(send_block[0, 0].T),
        hbm(send_target[0, 0].T),
        hbm(send_count[0]),
        hbm(send_weight[0, 0].reshape(peers * cap, cells, cells)),
        hbm(left_block[0, 0].T),
        hbm(left_target[0, 0].T),
        hbm(left_count[0]),
        hbm(left_weight[0, 0].reshape(levels * lcap, cells, cells)),
    )
    message = lax.all_to_all(
        message.reshape(devices * plan.rows // 2, 2, cells),
        ("level", "dev"),
        split_axis=0,
        concat_axis=0,
        tiled=True,
    ).reshape(plan.total, cells)
    remapped, totals = pl.pallas_call(
        functools.partial(second_kernel, plan),
        out_shape=(
            jax.ShapeDtypeStruct((rows, cells), jnp.float32),
            jax.ShapeDtypeStruct((comp,), jnp.float32),
        ),
        in_specs=[vmem, vmem, vmem],
        out_specs=(vmem, vmem),
        compiler_params=pltpu.CompilerParams(vmem_limit_bytes=24 * 2**20),
        name="place",
    )(own, message, place)
    remapped = remapped.reshape(comp, blocks, cells).transpose(1, 0, 2)
    return (remapped[None], totals)


def solution(mesh):
    in_specs = (
        P("level", "dev", None, None),
        P("level", "dev"),
        P("level", "dev", None, None),
        P("level", "dev", None, None),
        P("level", "dev", None, None),
        P("level", "dev", None),
        P("level", "dev", None, None, None, None),
        P("level", "dev", None, None),
        P("level", "dev", None, None),
        P("level", "dev", None),
        P("level", "dev", None, None, None, None),
    )
    out_specs = (P("level", "dev", None, None), P())
    return jax.shard_map(body, mesh=mesh, in_specs=in_specs, out_specs=out_specs, check_vma=False)
```

```python
import functools

import jax
import jax.numpy as jnp
from jax import lax
from jax.experimental import pallas as pl
from jax.experimental.pallas import tpu as pltpu
from jax.sharding import PartitionSpec as P

LANES = 128
TILE = 16


def up(value, step):
    return -(-value // step) * step


def divide(x, n, bound):
    if n & (n - 1) == 0:
        return x >> (n.bit_length() - 1)
    factor = -(-(1 << 20) // n)
    assert bound * (factor * n - (1 << 20)) < 1 << 20 and bound * factor < 1 << 31
    return (x * factor) >> 20


class Plan:
    def __init__(self, levels, peers, blocks, comp, cells, cap, lcap):
        self.levels, self.peers, self.blocks = levels, peers, blocks
        self.comp, self.cells, self.cap = comp, cells, cap
        self.data = cap * comp
        self.rows = self.data + 2
        self.ahead = peers * self.rows
        self.total = levels * self.ahead
        self.ids = (peers + levels) * cap
        self.window = up(self.rows + TILE - 2, TILE)
        self.picked = self.ahead + levels * self.window
        self.groups = -(-self.picked // LANES)
        assert cap == lcap and comp <= TILE and cells == LANES
        assert self.ahead % TILE == 0 and self.ids <= LANES
        assert self.rows % 2 == 0 and 2 * TILE + comp <= LANES

    def window_of(self, dev):
        first = (dev * self.rows) // TILE * TILE
        return pl.multiple_of(jnp.minimum(first, self.ahead - self.window), TILE)

    def slot_of(self, row):
        slot = jnp.zeros_like(row)
        for c in range(1, self.cap):
            slot += jnp.where(row >= c * self.comp, 1, 0)
        return slot


def first_kernel(
    plan,
    fields_hbm,
    own_src_hbm,
    own_weight_hbm,
    send_block_hbm,
    send_target_hbm,
    send_count_hbm,
    send_weight_hbm,
    left_block_hbm,
    left_target_hbm,
    left_count_hbm,
    left_weight_hbm,
    own_ref,
    msg_ref,
    place_ref,
    fields_v,
    donors,
    own_weight,
    send_weight,
    left_weight,
    wide,
    own_src,
    send_block,
    send_target,
    send_count,
    left_block,
    left_target,
    left_count,
    sems,
):
    blocks, comp, cap = plan.blocks, plan.comp, plan.cap
    pairs = (
        (fields_hbm, fields_v),
        (own_src_hbm, own_src),
        (send_block_hbm, send_block),
        (send_target_hbm, send_target),
        (send_count_hbm, send_count),
        (left_block_hbm, left_block),
        (left_target_hbm, left_target),
        (left_count_hbm, left_count),
        (send_weight_hbm, send_weight),
        (left_weight_hbm, left_weight),
        (own_weight_hbm, own_weight),
    )
    copies = [pltpu.make_async_copy(src, dst, sems.at[i]) for i, (src, dst) in enumerate(pairs)]
    for copy in copies:
        copy.start()

    level = lax.axis_index("level")
    dev = lax.axis_index("dev")

    lane = lax.broadcasted_iota(jnp.int32, (1, LANES), 1)
    skip = dev * plan.rows - plan.window_of(dev)
    for g in range(plan.groups):
        at = lane + g * LANES
        peer = divide(at, plan.rows, plan.picked + LANES)
        row = at - peer * plan.rows
        beyond = jnp.maximum(at - plan.ahead, 0)
        donor_level = divide(beyond, plan.window, plan.picked + LANES)
        other_row = beyond - donor_level * plan.window - skip
        row = jnp.where(at < plan.ahead, row, other_row)
        donor = jnp.where(at < plan.ahead, peer, plan.peers + donor_level)
        slot = plan.slot_of(row)
        live = (row >= 0) & (row < plan.data) & (at < plan.picked)
        place_ref[g : g + 1, :] = jnp.where(live, donor * cap + slot, 0)
        place_ref[plan.groups + g : plan.groups + g + 1, :] = jnp.where(
            live, row - slot * comp, -1
        )
    wide[...] = jnp.zeros_like(wide)

    copies[0].wait()
    donors[...] = jnp.zeros_like(donors)
    for b in range(blocks):
        donors[b, 0:comp, :] = fields_v[pl.ds(b, comp, stride=blocks), :].astype(jnp.bfloat16)
    for copy in copies[1:10]:
        copy.wait()

    row = lax.broadcasted_iota(jnp.int32, (TILE, LANES), 0)
    column = lax.broadcasted_iota(jnp.int32, (TILE, LANES), 1)

    empty = jnp.zeros((TILE, LANES), jnp.bfloat16)

    def terms(which, weights):
        count = len(which)
        rows = [
            jnp.concatenate([donors[b] if i == j else empty for j in range(count)], axis=1)
            for i, b in enumerate(which)
        ]
        out = jnp.dot(
            jnp.concatenate(rows, axis=0),
            weights.reshape(count * LANES, LANES),
            preferred_element_type=jnp.float32,
        )
        return [out[i * TILE : (i + 1) * TILE] for i in range(count)]

    sums = jnp.zeros((TILE, LANES), jnp.float32)
    for count, block, target, weight, peers, here, message_of, copy in (
        (
            send_count,
            send_block,
            send_target,
            send_weight,
            plan.peers,
            dev,
            lambda p: level * plan.peers + p,
            copies[8],
        ),
        (
            left_count,
            left_block,
            left_target,
            left_weight,
            plan.levels,
            plan.peers + level,
            lambda p: p * plan.peers + dev,
            copies[9],
        ),
    ):
        for p in range(peers):
            first = message_of(p) * plan.rows
            targets = jnp.zeros((1, LANES), jnp.float32)
            which = [jnp.where(c < count[0, p], block[c, p], blocks) for c in range(cap)]
            values = terms(which, weight[p * cap : (p + 1) * cap])
            for c, value in enumerate(values):
                sums += value
                wide[pl.ds(first + c * comp, comp), :] = value[0:comp]
                targets = jnp.where(
                    lane == here * cap + c, target[c, p].astype(jnp.float32), targets
                )
            wide[pl.ds(first + plan.data, 1), :] = targets
    copies[10].wait()
    for first in range(0, blocks, 2):
        which = range(first, min(first + 2, blocks))
        values = terms([own_src[0, b] for b in which], own_weight[first : which.stop])
        for b, mine in zip(which, values):
            sums += mine
            own_ref[pl.ds(b, comp, stride=blocks), :] = mine[0:comp]

    total = jnp.sum(sums, axis=1, keepdims=True)
    high = total.astype(jnp.bfloat16).astype(jnp.float32)
    rest = total - high
    middle = rest.astype(jnp.bfloat16).astype(jnp.float32)
    low = rest - middle
    spread = jnp.where(column == row, high, 0.0)
    spread = jnp.where(column == row + TILE, middle, spread)
    spread = jnp.where(column == row + 2 * TILE, low, spread)
    sum_row = jnp.sum(spread, axis=0, keepdims=True)
    for index in range(plan.levels * plan.peers):
        at = index * plan.rows + plan.data + 1
        wide[at : at + 1, :] = sum_row
    msg_ref[...] = wide[...].astype(jnp.bfloat16)


def second_kernel(plan, own_ref, msg_ref, place_ref, out_ref, totals_ref, picked):
    blocks, comp = plan.blocks, plan.comp
    mine = pl.multiple_of(lax.axis_index("level") * plan.ahead, TILE)
    picked[0 : plan.ahead, :] = msg_ref[pl.ds(mine, plan.ahead), :]
    first = plan.window_of(lax.axis_index("dev"))
    for donor_level in range(plan.levels):
        at = plan.ahead + donor_level * plan.window
        picked[at : at + plan.window, :] = msg_ref[
            pl.ds(pl.multiple_of(donor_level * plan.ahead + first, TILE), plan.window), :
        ]
    spans = [
        (g, g * LANES, min(LANES, plan.picked - g * LANES)) for g in range(plan.groups)
    ]

    found = {}
    for peer in range(plan.peers):
        at = peer * plan.rows + plan.data
        low = at // 8 * 8
        for donor_level in range(plan.levels):
            first = donor_level * plan.ahead + low
            part = msg_ref[first : first + 8, :].astype(jnp.float32)
            found[at - low] = found[at - low] + part if at - low in found else part
    meta = sum(part[at : at + 2, :] for at, part in found.items())

    targets = jnp.broadcast_to(meta[0:1, :], (blocks, LANES))
    block_row = lax.broadcasted_iota(jnp.int32, (blocks, LANES), 0).astype(jnp.float32)
    placed = own_ref[...]
    for g, at, size in spans:
        index = jnp.broadcast_to(place_ref[g : g + 1, :], (blocks, LANES))
        match = jnp.take_along_axis(targets, index, axis=1) == block_row
        at_part = plan.groups + g
        part = jnp.broadcast_to(place_ref[at_part : at_part + 1, :], (blocks, LANES))
        key = jnp.where(match, part, -1)
        select = jnp.concatenate(
            [jnp.where(key == m, 1.0, 0.0).astype(jnp.bfloat16) for m in range(comp)], axis=0
        )
        placed += jnp.dot(
            select[:, :size], picked[at : at + size, :], preferred_element_type=jnp.float32
        )
    out_ref[...] = placed

    sums = meta[1:2, :]
    total = sums[:, 0:comp]
    total += sums[:, TILE : TILE + comp]
    total += sums[:, 2 * TILE : 2 * TILE + comp]
    totals_ref[...] = (total * (1.0 / (plan.cells * blocks)))[0]


def hbm(x):
    return pltpu.with_memory_space_constraint(x, pltpu.HBM)


def body(
    fields,
    own_src,
    own_weight,
    send_block,
    send_target,
    send_count,
    send_weight,
    left_block,
    left_target,
    left_count,
    left_weight,
):
    blocks, comp, cells = fields.shape[1:]
    peers, cap = send_block.shape[2:]
    levels, lcap = left_block.shape[2:]
    plan = Plan(levels, peers, blocks, comp, cells, cap, lcap)
    rows = comp * blocks
    devices = levels * peers
    in_hbm = pl.BlockSpec(memory_space=pltpu.HBM)
    vmem = pl.BlockSpec(memory_space=pltpu.VMEM)
    own, message, place = pl.pallas_call(
        functools.partial(first_kernel, plan),
        out_shape=(
            jax.ShapeDtypeStruct((rows, cells), jnp.float32),
            jax.ShapeDtypeStruct((plan.total, cells), jnp.bfloat16),
            jax.ShapeDtypeStruct((2 * plan.groups, LANES), jnp.int32),
        ),
        in_specs=[in_hbm] * 11,
        out_specs=(vmem, vmem, vmem),
        scratch_shapes=[
            pltpu.VMEM((rows, cells), jnp.float32),
            pltpu.VMEM((blocks + 1, TILE, cells), jnp.bfloat16),
            pltpu.VMEM((blocks, cells, cells), jnp.bfloat16),
            pltpu.VMEM((peers * cap, cells, cells), jnp.bfloat16),
            pltpu.VMEM((levels * lcap, cells, cells), jnp.bfloat16),
            pltpu.VMEM((plan.total, cells), jnp.float32),
            pltpu.SMEM((1, blocks), jnp.int32),
            pltpu.SMEM((cap, peers), jnp.int32),
            pltpu.SMEM((cap, peers), jnp.int32),
            pltpu.SMEM((1, peers), jnp.int32),
            pltpu.SMEM((lcap, levels), jnp.int32),
            pltpu.SMEM((lcap, levels), jnp.int32),
            pltpu.SMEM((1, levels), jnp.int32),
            pltpu.SemaphoreType.DMA((11,)),
        ],
        compiler_params=pltpu.CompilerParams(vmem_limit_bytes=24 * 2**20),
        name="terms",
    )(
        hbm(fields[0].transpose(1, 0, 2).reshape(rows, cells)),
        hbm(own_src),
        hbm(own_weight[0]),
        hbm(send_block[0, 0].T),
        hbm(send_target[0, 0].T),
        hbm(send_count[0]),
        hbm(send_weight[0, 0].reshape(peers * cap, cells, cells)),
        hbm(left_block[0, 0].T),
        hbm(left_target[0, 0].T),
        hbm(left_count[0]),
        hbm(left_weight[0, 0].reshape(levels * lcap, cells, cells)),
    )
    message = lax.all_to_all(
        message.reshape(devices * plan.rows // 2, 2, cells),
        ("level", "dev"),
        split_axis=0,
        concat_axis=0,
        tiled=True,
    ).reshape(plan.total, cells)
    remapped, totals = pl.pallas_call(
        functools.partial(second_kernel, plan),
        out_shape=(
            jax.ShapeDtypeStruct((rows, cells), jnp.float32),
            jax.ShapeDtypeStruct((comp,), jnp.float32),
        ),
        in_specs=[vmem, vmem, vmem],
        out_specs=(vmem, vmem),
        scratch_shapes=[pltpu.VMEM((plan.picked, cells), jnp.bfloat16)],
        compiler_params=pltpu.CompilerParams(vmem_limit_bytes=24 * 2**20),
        name="place",
    )(own, message, place)
    remapped = remapped.reshape(comp, blocks, cells).transpose(1, 0, 2)
    return (remapped[None], totals)


def solution(mesh):
    in_specs = (
        P("level", "dev", None, None),
        P("level", "dev"),
        P("level", "dev", None, None),
        P("level", "dev", None, None),
        P("level", "dev", None, None),
        P("level", "dev", None),
        P("level", "dev", None, None, None, None),
        P("level", "dev", None, None),
        P("level", "dev", None, None),
        P("level", "dev", None),
        P("level", "dev", None, None, None, None),
    )
    out_specs = (P("level", "dev", None, None), P())
    return jax.shard_map(body, mesh=mesh, in_specs=in_specs, out_specs=out_specs, check_vma=False)
```
